8 devices in a mesh: dp: 2 (over y, z), tp: 4 (over x, core).
Axes of the slice: x: 2, y: 2, z: 1, core: 2. Of those that a mesh axis runs over, the one named last changes fastest.
Arguments:
- x: bfloat16 [2048, 4096], P(('dp', 'tp')), parts along dimension 0
- w_gate: bfloat16 [4096, 16384], P(None, 'tp')
- w_up: bfloat16 [4096, 16384], P(None, 'tp')
- w_down: bfloat16 [16384, 4096], P('tp')
Outputs:
- output: bfloat16 [2048, 4096], P(('dp', 'tp')), parts along dimension 0
There are 2 independent parts. The reference program is written for one: setup_inputs(seed, part) draws one part's arguments, and reference() takes and returns one part's arrays. A program takes and returns all parts, laid end to end along the dimension named above; an argument that names none is the same for every part.
All inputs are finite; a program needn't handle non-finite values.
Results may differ from the reference program's by a relative error of at most 0.016.
Values are sent between devices in bfloat16 or wider.
A program may use at most 2 GiB of HBM per device.

```python
import jax
import jax.numpy as jnp

ROWS = 1024
D = 4096
FF = 16384


def setup_inputs(seed: int = 0, part: int = 0) -> dict:
    kx, kg, ku, kd = jax.random.split(jax.random.key(seed), 4)
    drawn = {
        "x": jax.random.normal(jax.random.fold_in(kx, part), (ROWS, D), jnp.float32),
        "w_gate": jax.random.normal(kg, (D, FF), jnp.float32) * D**-0.5,
        "w_up": jax.random.normal(ku, (D, FF), jnp.float32) * D**-0.5,
        "w_down": jax.random.normal(kd, (FF, D), jnp.float32) * FF**-0.5,
    }
    return {k: v.astype(jnp.bfloat16) for k, v in drawn.items()}


def reference(x, w_gate, w_up, w_down):
    gate = jnp.dot(x, w_gate, preferred_element_type=jnp.float32)
    up = jnp.dot(x, w_up, preferred_element_type=jnp.float32)
    hidden = (jax.nn.silu(gate) * up).astype(jnp.bfloat16)
    return jnp.dot(hidden, w_down, preferred_element_type=jnp.float32).astype(jnp.bfloat16)
```

```python
import jax
import jax.numpy as jnp
from jax import lax
from jax.experimental import pallas as pl
from jax.experimental.pallas import tpu as pltpu
from jax.sharding import PartitionSpec as P

MESH = pl.DeviceIdType.MESH
BF16, F32 = jnp.bfloat16, jnp.float32
D = 4096
ROWS = 256
HALF = ROWS // 2
T = 256
GU, DN = D // T, D // (2 * T)
SLOTS = 8
PRE = SLOTS - 1
OWN_ONLY = 3
LATE = 12
N1 = GU
N2 = N1 + LATE
N3 = N2 + DN
N4 = N3 + GU
N5 = N4 + DN
N6 = N5 + DN


def dot(a, b):
    return jnp.dot(a, b, preferred_element_type=F32)


def kernel(
    x_hbm, wg_hbm, wu_hbm, wd_hbm, y_hbm,
    xv, hid, ring, keep, stage, drecv, yrecv, pstage, okeep, ostage,
    wsem, xsem, osem, ag_send, ag_recv, d_send, d_recv, i_send, i_recv, p_send, p_recv,
):
    dp, tp = lax.axis_index("dp"), lax.axis_index("tp")
    chip, core = tp // 2, tp % 2
    mate = (dp, chip * 2 + 1 - core)
    peer = (dp, (1 - chip) * 2 + core)

    def remote(src, dst, send, recv, to):
        return pltpu.make_async_remote_copy(
            src_ref=src, dst_ref=dst, send_sem=send, recv_sem=recv, device_id=to, device_id_type=MESH
        )

    def tile(ref, t, slot, which):
        return pltpu.make_async_copy(
            ref.at[:, pl.ds(pl.multiple_of(t * T, T), T)], ring.at[slot, which], wsem.at[slot, which]
        )

    def fetch_gu(q, t):
        slot = lax.rem(q, SLOTS)
        tile(wg_hbm, t, slot, 0).start()
        tile(wu_hbm, t, slot, 1).start()

    def fetch_dn(q, n):
        slot = lax.rem(q, SLOTS)
        tile(wd_hbm, 2 * n, slot, 0).start()
        tile(wd_hbm, 2 * n + 1, slot, 1).start()

    def fetch(q):
        first = q < N2
        third = jnp.logical_and(q >= N3, q < N4)

        @pl.when(first)
        def _():
            fetch_gu(q, lax.rem(q, GU))

        @pl.when(third)
        def _():
            fetch_gu(q, q - N3)

        @pl.when(jnp.logical_and(q >= N2, q < N3))
        def _():
            fetch_dn(q, q - N2)

        @pl.when(jnp.logical_and(q >= N4, q < N6))
        def _():
            fetch_dn(q, lax.rem(q - N4, DN))

    def arrive(q):
        slot = lax.rem(q, SLOTS)
        tile(wg_hbm, 0, slot, 0).wait()
        tile(wg_hbm, 0, slot, 1).wait()
        fetch(q + PRE)
        return slot

    def gate_up(slot, t, lo, hi, out):
        col = pl.ds(pl.multiple_of(t * T, T), T)
        for r in range(lo, hi, ROWS):
            gate = dot(xv[r : r + ROWS, :], ring[slot, 0])
            up = dot(xv[r : r + ROWS, :], ring[slot, 1])
            hid[out + r - lo : out + r - lo + ROWS, col] = (jax.nn.silu(gate) * up).astype(BF16)

    own = pltpu.make_async_copy(x_hbm, xv.at[pl.ds(0, ROWS)], xsem)
    own.start()
    fetch_gu(0, 0)
    fetch_gu(1, 1)
    barrier = pltpu.get_barrier_semaphore()
    for to in (mate, peer):
        pl.semaphore_signal(barrier, inc=1, device_id=to, device_id_type=MESH)
    pl.semaphore_wait(barrier, 2)
    near = remote(x_hbm, xv.at[pl.ds(ROWS, ROWS)], ag_send.at[0], ag_recv.at[0], mate)
    near.start()

    def far(h):
        return remote(
            x_hbm.at[pl.ds(h * HALF, HALF)],
            xv.at[pl.ds((2 + h) * ROWS, HALF)],
            ag_send.at[1 + h], ag_recv.at[1 + h], peer,
        )

    def forward(h):
        return remote(
            xv.at[pl.ds((2 + h) * ROWS, HALF)],
            xv.at[pl.ds((2 + h) * ROWS + HALF, HALF)],
            ag_send.at[3 + h], ag_recv.at[3 + h], mate,
        )

    far(0).start()
    far(1).start()
    for q in range(2, PRE):
        fetch_gu(q, q)
    own.wait()

    def pass_own(t, _):
        slot = arrive(t)
        gate_up(slot, t, 0, ROWS, 0)
        return 0

    lax.fori_loop(0, OWN_ONLY, pass_own, 0)
    near.wait_recv()

    def pass_near(t, _):
        @pl.when(t == LATE - 1)
        def _():
            far(0).wait_recv()
            forward(0).start()

        slot = arrive(t)
        gate_up(slot, t, 0, 2 * ROWS, 0)
        return 0

    lax.fori_loop(OWN_ONLY, LATE, pass_near, 0)
    near.wait_send()
    forward(0).wait()

    def pass_three(t, _):
        slot = arrive(t)
        gate_up(slot, t, 0, 3 * ROWS, 0)
        return 0

    lax.fori_loop(LATE, GU, pass_three, 0)

    def pass_mixed(t, _):
        slot = arrive(t + N1)
        gate_up(slot, t, ROWS, 3 * ROWS, ROWS)
        return 0

    lax.fori_loop(0, OWN_ONLY, pass_mixed, 0)

    def pass_far(t, _):
        slot = arrive(t + N1)
        gate_up(slot, t, 2 * ROWS, 3 * ROWS, 2 * ROWS)
        return 0

    lax.fori_loop(OWN_ONLY, LATE, pass_far, 0)
    far(1).wait_recv()
    forward(1).start()

    def to_mate(h, n):
        k = h * DN + n
        return remote(stage.at[lax.rem(n, 4)], drecv.at[k], d_send.at[k], d_recv.at[k], mate)

    def to_peer(h, n):
        k = h * DN + n
        return remote(drecv.at[k], yrecv.at[k], i_send.at[k], i_recv.at[k], peer)

    def tick(h, n):
        @pl.when(jnp.logical_and(n >= 1, n <= DN))
        def _():
            to_mate(h, n - 1).start()

        @pl.when(jnp.logical_and(n >= 3, n <= DN + 2))
        def _():
            to_peer(h, n - 3).start()

        @pl.when(jnp.logical_and(n >= 2, n <= DN + 1))
        def _():
            m = n - 2
            to_mate(h, m).wait()
            k = h * DN + m
            drecv[k] = (keep[lax.rem(m, 4)] + drecv[k].astype(F32)).astype(BF16)

    def down_far(h, base):
        def body(n, _):
            tick(h, n)
            slot = arrive(base + n)
            for w in range(2):
                term = dot(hid[2 * ROWS :, :], ring[slot, w])
                keep[lax.rem(n, 4), :, w * T : (w + 1) * T] = term[:HALF]
                stage[lax.rem(n, 4), :, w * T : (w + 1) * T] = term[HALF:].astype(BF16)
            return 0

        lax.fori_loop(0, DN, body, 0)

    down_far(0, N2)
    forward(1).wait()
    far(0).wait_send()
    far(1).wait_send()

    def pass_last(t, _):
        tick(0, t + DN)
        slot = arrive(t + N3)
        gate_up(slot, t, 3 * ROWS, 4 * ROWS, 2 * ROWS)
        return 0

    lax.fori_loop(0, GU, pass_last, 0)
    down_far(1, N4)

    def columns(n):
        return pl.ds(pl.multiple_of(n * 2 * T, 2 * T), 2 * T)

    def rows_to_mate(n):
        return remote(
            pstage.at[lax.rem(n, 4)],
            xv.at[pl.ds(2 * ROWS, ROWS), columns(n)],
            p_send.at[n], p_recv.at[n], mate,
        )

    def write(n):
        s = lax.rem(n, 2)
        return pltpu.make_async_copy(ostage.at[s], y_hbm.at[:, columns(n)], osem.at[s])

    def finish(n):
        rows_to_mate(n).wait()
        to_peer(0, n).wait_recv()
        to_peer(1, n).wait_recv()
        near_term = xv[2 * ROWS : 3 * ROWS, columns(n)].astype(F32)
        s = lax.rem(n, 4)
        for h in range(2):
            r = slice(h * HALF, (h + 1) * HALF)
            total = okeep[s, r] + near_term[r] + yrecv[h * DN + n].astype(F32)
            ostage[lax.rem(n, 2), r] = total.astype(BF16)
        write(n).start()

    def down_near(n, _):
        @pl.when(n >= 1)
        def _():
            rows_to_mate(n - 1).start()

        tick(1, n + DN)

        @pl.when(n >= 4)
        def _():
            write(n - 4).wait()

        @pl.when(n >= 2)
        def _():
            finish(n - 2)

        slot = arrive(N5 + n)
        s = lax.rem(n, 4)
        for w in range(2):
            c = slice(w * T, (w + 1) * T)
            pstage[s, :, c] = dot(hid[ROWS : 2 * ROWS, :], ring[slot, w]).astype(BF16)
        for w in range(2):
            c = slice(w * T, (w + 1) * T)
            okeep[s, :, c] = dot(hid[:ROWS, :], ring[slot, w])
        return 0

    lax.fori_loop(0, DN, down_near, 0)
    rows_to_mate(DN - 1).start()
    for n in (DN - 2, DN - 1):
        write(n - 2).wait()
        finish(n)
    for n in (DN - 2, DN - 1):
        write(n).wait()

    for h in range(2):

        def drain(n, _):
            to_peer(h, n).wait_send()
            return 0

        lax.fori_loop(0, DN, drain, 0)


def solution(mesh):
    def step(x, w_gate, w_up, w_down):
        dma = pltpu.SemaphoreType.DMA
        return pl.pallas_call(
            kernel,
            out_shape=jax.ShapeDtypeStruct((ROWS, D), BF16),
            in_specs=[pl.BlockSpec(memory_space=pltpu.HBM)] * 4,
            out_specs=pl.BlockSpec(memory_space=pltpu.HBM),
            scratch_shapes=[
                pltpu.VMEM((4 * ROWS, D), BF16),
                pltpu.VMEM((3 * ROWS, D), BF16),
                pltpu.VMEM((SLOTS, 2, D, T), BF16),
                pltpu.VMEM((4, HALF, 2 * T), F32),
                pltpu.VMEM((4, HALF, 2 * T), BF16),
                pltpu.VMEM((2 * DN, HALF, 2 * T), BF16),
                pltpu.VMEM((2 * DN, HALF, 2 * T), BF16),
                pltpu.VMEM((4, ROWS, 2 * T), BF16),
                pltpu.VMEM((4, ROWS, 2 * T), F32),
                pltpu.VMEM((2, ROWS, 2 * T), BF16),
                dma((SLOTS, 2)),
                dma,
                dma((2,)),
                dma((5,)),
                dma((5,)),
                dma((2 * DN,)),
                dma((2 * DN,)),
                dma((2 * DN,)),
                dma((2 * DN,)),
                dma((DN,)),
                dma((DN,)),
            ],
            compiler_params=pltpu.CompilerParams(
                collective_id=0, has_side_effects=True, vmem_limit_bytes=67043328
            ),
            name="mlp",
        )(x, w_gate, w_up, w_down)

    return jax.shard_map(
        step,
        mesh=mesh,
        in_specs=(P(("dp", "tp"), None), P(None, "tp"), P(None, "tp"), P("tp", None)),
        out_specs=P(("dp", "tp"), None),
        check_vma=False,
    )
```

```python
import jax
import jax.numpy as jnp
from jax import lax
from jax.experimental import pallas as pl
from jax.experimental.pallas import tpu as pltpu
from jax.sharding import PartitionSpec as P

MESH = pl.DeviceIdType.MESH
BF16, F32 = jnp.bfloat16, jnp.float32
D = 4096
ROWS = 256
HALF = ROWS // 2
T = 256
W = 2 * T
GU, DN = D // T, D // W
SLOTS = 8
LEFT = 2
LATE = GU - 2
PASS = GU + DN
REST = LATE + 2 * PASS
LAST = REST + GU - LATE + LEFT
O, M, R = 0, ROWS, 2 * ROWS


def dot(a, b):
    return jnp.dot(a, b, preferred_element_type=F32)


def kernel(
    x_hbm, wg_hbm, wu_hbm, wd_hbm, y_hbm,
    xv, hid, ring, keep, stage, drecv, yrecv, ostage,
    wsem, xsem, osem, ag_send, ag_recv, d_send, d_recv, i_send, i_recv, p_send, p_recv,
):
    dp, tp = lax.axis_index("dp"), lax.axis_index("tp")
    chip, core = tp // 2, tp % 2
    mate = (dp, chip * 2 + 1 - core)
    peer = (dp, (1 - chip) * 2 + core)

    def remote(src, dst, send, recv, to):
        return pltpu.make_async_remote_copy(
            src_ref=src, dst_ref=dst, send_sem=send, recv_sem=recv, device_id=to, device_id_type=MESH
        )

    def tile(ref, t, slot, which):
        return pltpu.make_async_copy(
            ref.at[:, pl.ds(pl.multiple_of(t * T, T), T)], ring.at[slot, which], wsem.at[slot, which]
        )

    def fetch_gu(q, t):
        slot = lax.rem(q, SLOTS)
        tile(wg_hbm, t, slot, 0).start()
        tile(wu_hbm, t, slot, 1).start()

    def fetch_dn(q, n):
        slot = lax.rem(q, SLOTS)
        tile(wd_hbm, 2 * n, slot, 0).start()
        tile(wd_hbm, 2 * n + 1, slot, 1).start()

    def arrive(q):
        slot = lax.rem(q, SLOTS)
        tile(wg_hbm, 0, slot, 0).wait()
        tile(wg_hbm, 0, slot, 1).wait()

    def gate_up(q, t, row, out):
        slot = lax.rem(q, SLOTS)
        x = xv[pl.ds(row, ROWS), :]
        gate = dot(x, ring[slot, 0])
        up = dot(x, ring[slot, 1])
        hid[pl.ds(out, ROWS), pl.ds(pl.multiple_of(t * T, T), T)] = (jax.nn.silu(gate) * up).astype(BF16)

    own = pltpu.make_async_copy(x_hbm, xv.at[pl.ds(O, ROWS)], xsem)
    own.start()
    fetch_gu(0, 0)
    fetch_gu(1, 1)
    barrier = pltpu.get_barrier_semaphore()
    for to in (mate, peer):
        pl.semaphore_signal(barrier, inc=1, device_id=to, device_id_type=MESH)
    pl.semaphore_wait(barrier, 2)
    near = remote(x_hbm, xv.at[pl.ds(M, ROWS)], ag_send.at[0], ag_recv.at[0], mate)
    near.start()

    def far(h):
        return remote(
            x_hbm.at[pl.ds(h * HALF, HALF)], xv.at[pl.ds(R + h * ROWS, HALF)], ag_send.at[1 + h], ag_recv.at[1 + h], peer
        )

    def forward(h):
        return remote(
            xv.at[pl.ds(R + h * ROWS, HALF)],
            xv.at[pl.ds(R + h * ROWS + HALF, HALF)],
            ag_send.at[3 + h], ag_recv.at[3 + h], mate,
        )

    far(0).start()
    far(1).start()
    for q in range(2, SLOTS):
        fetch_gu(q, q)
    own.wait()

    def pass_own(q, _):
        arrive(q)
        gate_up(q, q, O, O)
        fetch_gu(q + SLOTS, q + SLOTS)
        return 0

    lax.fori_loop(0, LEFT, pass_own, 0)
    near.wait()

    def pass_near(j, _):
        q = LEFT + 2 * j

        @pl.when(j == (LATE - LEFT) // 2 - 1)
        def _():
            far(0).wait_recv()
            forward(0).start()

        for u in range(2):
            arrive(q + u)
        for u in range(2):
            gate_up(q + u, q + u, O, O)
            gate_up(q + u, q + u, M, M)
        for u in range(2):
            fetch_gu(q + u + SLOTS, lax.rem(q + u + SLOTS, LATE))
        return 0

    lax.fori_loop(0, (LATE - LEFT) // 2, pass_near, 0)
    forward(0).wait()

    def to_mate(h, n):
        k = h * DN + n
        return remote(stage.at[lax.rem(n, 4), pl.ds(0, HALF)], drecv.at[k], d_send.at[k], d_recv.at[k], mate)

    def to_peer(h, n):
        k = h * DN + n
        return remote(drecv.at[k], yrecv.at[k], i_send.at[k], i_recv.at[k], peer)

    def combine(h, d):
        for u in range(2):
            n = 2 * d + u
            to_mate(h, n).wait()
            k = h * DN + n
            drecv[k] = (keep[lax.rem(n, 6), :HALF] + drecv[k].astype(F32)).astype(BF16)

    def send_terms(h, d):
        for u in range(2):
            to_mate(h, 2 * d + u).start()

    def send_sums(h, d):
        for u in range(2):
            to_peer(h, 2 * d + u).start()

    def tail(h, j):
        @pl.when(j == 0)
        def _():
            send_terms(h, 3)
            combine(h, 2)
            send_sums(h, 2)

        @pl.when(j == 1)
        def _():
            combine(h, 3)
            send_sums(h, 3)

    def half(h, _):
        base = LATE + PASS * h
        row = pl.multiple_of(R + h * ROWS, ROWS)

        def gate_up_far(j, _):
            q = base + 2 * j

            @pl.when(jnp.logical_and(h == 1, j < 2))
            def _():
                tail(0, j)

            for u in range(2):
                arrive(q + u)
            for u in range(2):
                gate_up(q + u, 2 * j + u, row, R)

            @pl.when(j < 4)
            def _():
                for u in range(2):
                    fetch_gu(q + u + SLOTS, 2 * j + u + SLOTS)

            @pl.when(j >= 4)
            def _():
                for u in range(2):
                    fetch_dn(q + u + SLOTS, 2 * j + u + SLOTS - GU)

            return 0

        lax.fori_loop(0, GU // 2, gate_up_far, 0)

        @pl.when(h == 0)
        def _():
            far(1).wait_recv()
            forward(1).start()

        def down_far(d, _):
            q = base + GU + 2 * d

            @pl.when(d >= 1)
            def _():
                send_terms(h, d - 1)

            @pl.when(d >= 2)
            def _():
                combine(h, d - 2)
                send_sums(h, d - 2)

            for u in range(2):
                arrive(q + u)
            for u in range(2):
                slot, n = lax.rem(q + u, SLOTS), 2 * d + u
                for w in range(2):
                    c = slice(w * T, (w + 1) * T)
                    term = dot(hid[R:, :], ring[slot, w])
                    keep[lax.rem(n, 6), :HALF, c] = term[:HALF]
                    stage[lax.rem(n, 4), :HALF, c] = term[HALF:].astype(BF16)

            @pl.when(h == 0)
            def _():
                for u in range(2):
                    fetch_gu(q + u + SLOTS, 2 * d + u)

            @pl.when(jnp.logical_and(h == 1, d < 2))
            def _():
                for u in range(2):
                    fetch_gu(q + u + SLOTS, lax.rem(LATE + 2 * d + u, GU))

            @pl.when(jnp.logical_and(h == 1, d >= 2))
            def _():
                for u in range(2):
                    fetch_dn(q + u + SLOTS, 2 * d + u - 4)

            return 0

        lax.fori_loop(0, DN // 2, down_far, 0)

        @pl.when(h == 0)
        def _():
            forward(1).wait()

        return 0

    lax.fori_loop(0, 2, half, 0)
    far(0).wait_send()
    far(1).wait_send()

    for j, (steps, rows) in enumerate(((range(LATE, GU), (O, M)), (range(LEFT), (M,)))):
        tail(1, j)
        q = REST + 2 * j
        for u in range(2):
            arrive(q + u)
        for u, t in enumerate(steps):
            for r in rows:
                gate_up(q + u, t, r, r)
        for u in range(2):
            fetch_dn(q + u + SLOTS, q + u + SLOTS - LAST)

    def columns(n):
        return pl.ds(pl.multiple_of(n * W, W), W)

    def rows_to_mate(n):
        return remote(
            stage.at[lax.rem(n, 4)], xv.at[pl.ds(R, ROWS), columns(n)], p_send.at[n], p_recv.at[n], mate
        )

    def send_rows(j):
        for u in range(2):
            rows_to_mate(2 * j + u).start()

    def take(j):
        for u in range(2):
            n = 2 * j + u
            rows_to_mate(n).wait()
            to_peer(0, n).wait_recv()
            to_peer(1, n).wait_recv()

    def total(j):
        for n in (2 * j, 2 * j + 1):
            for h in range(2):
                r = slice(h * HALF, (h + 1) * HALF)
                mates = xv[R + h * HALF : R + (h + 1) * HALF, n * W : (n + 1) * W].astype(F32)
                y = keep[n % 6, r] + mates + yrecv[h * DN + n].astype(F32)
                ostage[n % 4, r] = y.astype(BF16)

    def write(n):
        s = n % 4
        return pltpu.make_async_copy(ostage.at[s], y_hbm.at[:, pl.ds(n * W, W)], osem.at[s])

    def write_out(j):
        for u in range(2):
            write(2 * j + u).start()

    def written(j):
        for u in range(2):
            write(2 * j + u).wait()

    def mates_rows(j):
        for u in range(2):
            n = 2 * j + u
            slot = lax.rem(LAST + n, SLOTS)
            for w in range(2):
                stage[lax.rem(n, 4), :, w * T : (w + 1) * T] = dot(hid[M:R, :], ring[slot, w]).astype(BF16)

    def own_rows(j):
        for u in range(2):
            n = 2 * j + u
            slot = lax.rem(LAST + n, SLOTS)
            for w in range(2):
                keep[lax.rem(n, 6), :, w * T : (w + 1) * T] = dot(hid[O:M, :], ring[slot, w])

    def arrived(j):
        for u in range(2):
            arrive(LAST + 2 * j + u)

    def down_own(j, _):
        pl.when(j == 1)(lambda: send_rows(0))
        arrived(j)
        mates_rows(j)
        own_rows(j)
        return 0

    lax.fori_loop(0, 2, down_own, 0)
    send_rows(1)
    take(0)
    arrived(2)
    total(0)
    mates_rows(2)
    own_rows(2)

    send_rows(2)
    write_out(0)
    take(1)
    arrived(3)
    total(1)
    mates_rows(3)

    send_rows(3)
    write_out(1)
    take(2)
    written(0)
    total(2)
    own_rows(3)

    write_out(2)
    take(3)
    written(1)
    total(3)
    write_out(3)

    for h in range(2):

        def drain(n, _):
            to_peer(h, n).wait_send()
            return 0

        lax.fori_loop(0, DN, drain, 0)
    written(2)
    written(3)


def solution(mesh):
    def step(x, w_gate, w_up, w_down):
        dma = pltpu.SemaphoreType.DMA
        return pl.pallas_call(
            kernel,
            out_shape=jax.ShapeDtypeStruct((ROWS, D), BF16),
            in_specs=[pl.BlockSpec(memory_space=pltpu.HBM)] * 4,
            out_specs=pl.BlockSpec(memory_space=pltpu.HBM),
            scratch_shapes=[
                pltpu.VMEM((4 * ROWS, D), BF16),
                pltpu.VMEM((3 * ROWS, D), BF16),
                pltpu.VMEM((SLOTS, 2, D, T), BF16),
                pltpu.VMEM((6, ROWS, W), F32),
                pltpu.VMEM((4, ROWS, W), BF16),
                pltpu.VMEM((2 * DN, HALF, W), BF16),
                pltpu.VMEM((2 * DN, HALF, W), BF16),
                pltpu.VMEM((4, ROWS, W), BF16),
                dma((SLOTS, 2)),
                dma,
                dma((4,)),
                dma((5,)),
                dma((5,)),
                dma((2 * DN,)),
                dma((2 * DN,)),
                dma((2 * DN,)),
                dma((2 * DN,)),
                dma((DN,)),
                dma((DN,)),
            ],
            compiler_params=pltpu.CompilerParams(
                collective_id=0, has_side_effects=True, vmem_limit_bytes=67043328
            ),
            name="mlp",
        )(x, w_gate, w_up, w_down)

    return jax.shard_map(
        step,
        mesh=mesh,
        in_specs=(P(("dp", "tp"), None), P(None, "tp"), P(None, "tp"), P("tp", None)),
        out_specs=P(("dp", "tp"), None),
        check_vma=False,
    )
```

```python
import jax
import jax.numpy as jnp
from jax import lax
from jax.experimental import pallas as pl
from jax.experimental.pallas import tpu as pltpu
from jax.sharding import PartitionSpec as P

MESH = pl.DeviceIdType.MESH
BF16, F32 = jnp.bfloat16, jnp.float32
D = 4096
ROWS = 256
HALF = ROWS // 2
T = 256
W = 2 * T
GU, DN = D // T, D // W
SLOTS = 10
LEFT = 2
LATE = GU - 2
PASS = GU + DN
REST = LATE + 2 * PASS
LAST = REST + GU - LATE + LEFT
O, M, R = 0, ROWS, 2 * ROWS


def dot(a, b):
    return jnp.dot(a, b, preferred_element_type=F32)


def kernel(
    x_hbm, wg_hbm, wu_hbm, wd_hbm, y_hbm,
    xv, hid, ring, keep, stage, drecv, yrecv,
    wsem, xsem, osem, ag_send, ag_recv, d_send, d_recv, i_send, i_recv, p_send, p_recv, free,
):
    dp, tp = lax.axis_index("dp"), lax.axis_index("tp")
    chip, core = tp // 2, tp % 2
    mate = (dp, chip * 2 + 1 - core)
    peer = (dp, (1 - chip) * 2 + core)

    def remote(src, dst, send, recv, to):
        return pltpu.make_async_remote_copy(
            src_ref=src, dst_ref=dst, send_sem=send, recv_sem=recv, device_id=to, device_id_type=MESH
        )

    def tile(ref, t, slot, which):
        return pltpu.make_async_copy(
            ref.at[:, pl.ds(pl.multiple_of(t * T, T), T)], ring.at[slot, which], wsem.at[slot, which]
        )

    def fetch_gu(q, t):
        slot = lax.rem(q, SLOTS)
        tile(wg_hbm, t, slot, 0).start()
        tile(wu_hbm, t, slot, 1).start()

    def fetch_dn(q, n):
        slot = lax.rem(q, SLOTS)
        tile(wd_hbm, 2 * n, slot, 0).start()
        tile(wd_hbm, 2 * n + 1, slot, 1).start()

    def arrive(q):
        slot = lax.rem(q, SLOTS)
        tile(wg_hbm, 0, slot, 0).wait()
        tile(wg_hbm, 0, slot, 1).wait()

    def gate_up(q, t, row, out):
        slot = lax.rem(q, SLOTS)
        x = xv[pl.ds(row, ROWS), :]
        gate = dot(x, ring[slot, 0])
        up = dot(x, ring[slot, 1])
        hid[pl.ds(out, ROWS), pl.ds(pl.multiple_of(t * T, T), T)] = (jax.nn.silu(gate) * up).astype(BF16)

    own = pltpu.make_async_copy(x_hbm, xv.at[pl.ds(O, ROWS)], xsem)
    own.start()
    fetch_gu(0, 0)
    fetch_gu(1, 1)
    barrier = pltpu.get_barrier_semaphore()
    for to in (mate, peer):
        pl.semaphore_signal(barrier, inc=1, device_id=to, device_id_type=MESH)
    pl.semaphore_wait(barrier, 2)
    near = remote(x_hbm, xv.at[pl.ds(M, ROWS)], ag_send.at[0], ag_recv.at[0], mate)
    near.start()

    def far(h):
        return remote(
            x_hbm.at[pl.ds(h * HALF, HALF)], xv.at[pl.ds(R + h * ROWS, HALF)], ag_send.at[1 + h], ag_recv.at[1 + h], peer
        )

    def forward(h):
        return remote(
            xv.at[pl.ds(R + h * ROWS, HALF)],
            xv.at[pl.ds(R + h * ROWS + HALF, HALF)],
            ag_send.at[3 + h], ag_recv.at[3 + h], mate,
        )

    far(0).start()
    far(1).start()
    for q in range(2, SLOTS):
        fetch_gu(q, q)
    own.wait()

    def pass_own(q, _):
        arrive(q)
        gate_up(q, q, O, O)
        fetch_gu(q + SLOTS, q + SLOTS)
        return 0

    lax.fori_loop(0, LEFT, pass_own, 0)
    near.wait()

    def pass_near(q, u):
        for i in range(u):
            arrive(q + i)
        for i in range(u):
            gate_up(q + i, q + i, O, O)
            gate_up(q + i, q + i, M, M)
        for i in range(u):
            fetch_gu(q + i + SLOTS, lax.rem(q + i + SLOTS, LATE))

    def pass_single(q, _):
        pass_near(q, 1)
        return 0

    lax.fori_loop(LEFT, LEFT + 2, pass_single, 0)

    def pass_double(j, _):
        @pl.when(j == LATE // 2 - 1)
        def _():
            far(0).wait_recv()
            forward(0).start()

        pass_near(2 * j, 2)
        return 0

    lax.fori_loop(LEFT // 2 + 1, LATE // 2, pass_double, 0)
    forward(0).wait()

    def place(n, part):
        return pl.ds(R + ROWS + part * HALF, HALF), pl.ds(n * W, W)

    def terms(h, n):
        return xv.at[place(n, 0)] if h else drecv.at[n]

    def sums(h, n):
        return xv.at[place(n, 1)] if h else yrecv.at[n]

    def to_mate(h, d, i):
        n = 4 * d + i
        k = h * DN + n
        src = stage.at[2 * d + i // 2, pl.ds(i % 2 * HALF, HALF)]
        return remote(src, terms(h, n), d_send.at[k], d_recv.at[k], mate)

    def to_peer(h, n):
        k = h * DN + n
        return remote(terms(h, n), sums(h, n), i_send.at[k], i_recv.at[k], peer)

    def send_terms(h, d):
        for i in range(4):
            to_mate(h, d, i).start()

    def combine(h, d):
        for i in range(4):
            to_mate(h, d, i).wait()
        for i in range(4):
            at = terms(h, 4 * d + i)
            mine = keep[2 * d + i // 2, i % 2 * HALF : (i % 2 + 1) * HALF]
            at[...] = (mine + at[...].astype(F32)).astype(BF16)

    def send_sums(h, d):
        for i in range(4):
            to_peer(h, 4 * d + i).start()

    def half(h, _):
        base = LATE + PASS * h
        row = pl.multiple_of(R + h * ROWS, ROWS)

        def gate_up_far(j, _):
            q = base + 4 * j

            @pl.when(jnp.logical_and(h == 1, j == 0))
            def _():
                combine(0, 0)
                send_terms(0, 1)
                send_sums(0, 0)

            @pl.when(jnp.logical_and(h == 1, j == 1))
            def _():
                combine(0, 1)

            for i in range(4):
                arrive(q + i)

            @pl.when(jnp.logical_and(h == 1, j == 1))
            def _():
                send_sums(0, 1)

            for i in range(4):
                gate_up(q + i, 4 * j + i, row, R)

            @pl.when(j < 2)
            def _():
                for i in range(2):
                    fetch_gu(q + i + SLOTS, 4 * j + i + SLOTS)

            @pl.when(j >= 2)
            def _():
                for i in range(2):
                    fetch_dn(q + i + SLOTS, 4 * j + i + SLOTS - GU)

            @pl.when(j < 1)
            def _():
                for i in range(2, 4):
                    fetch_gu(q + i + SLOTS, 4 * j + i + SLOTS)

            @pl.when(jnp.logical_and(j >= 1, j < 3))
            def _():
                for i in range(2, 4):
                    fetch_dn(q + i + SLOTS, 4 * j + i + SLOTS - GU)

            @pl.when(j == 3)
            def _():
                for i in range(2):
                    fetch_gu(q + i + 2 + SLOTS, LATE * h + i)

            return 0

        lax.fori_loop(0, GU // 4, gate_up_far, 0)

        @pl.when(h == 0)
        def _():
            far(1).wait_recv()
            forward(1).start()

        @pl.when(h == 1)
        def _():
            for i, to in enumerate((mate, peer)):
                pl.semaphore_signal(free.at[i], inc=1, device_id=to, device_id_type=MESH)

        def down_far(d, _):
            q = base + GU + 4 * d

            @pl.when(jnp.logical_and(d == 1, h == 0))
            def _():
                send_terms(0, 0)

            @pl.when(jnp.logical_and(d == 1, h == 1))
            def _():
                pl.semaphore_wait(free.at[0], 1)
                send_terms(1, 0)

            for i in range(4):
                arrive(q + i)
            for i in range(4):
                slot = lax.rem(q + i, SLOTS)
                r = slice(i % 2 * HALF, (i % 2 + 1) * HALF)
                for w in range(2):
                    c = slice(w * T, (w + 1) * T)
                    term = dot(hid[R:, :], ring[slot, w])
                    keep[2 * d + i // 2, r, c] = term[:HALF]
                    stage[2 * d + i // 2, r, c] = term[HALF:].astype(BF16)

            @pl.when(h == 0)
            def _():
                for i in range(4):
                    fetch_gu(q + i + SLOTS, 4 * d + i + 2)

            @pl.when(jnp.logical_and(h == 1, d == 0))
            def _():
                for i in range(2):
                    fetch_gu(q + i + SLOTS, i)
                for i in range(2):
                    fetch_dn(q + i + 2 + SLOTS, i)

            @pl.when(jnp.logical_and(h == 1, d == 1))
            def _():
                for i in range(4):
                    fetch_dn(q + i + SLOTS, i + 2)

            return 0

        lax.fori_loop(0, DN // 4, down_far, 0)

        @pl.when(h == 0)
        def _():
            forward(1).wait()

        return 0

    lax.fori_loop(0, 2, half, 0)
    far(0).wait_send()
    far(1).wait_send()

    combine(1, 0)
    send_terms(1, 1)
    pl.semaphore_wait(free.at[1], 1)
    send_sums(1, 0)
    steps = (*range(LATE, GU), *range(LEFT))
    for i in range(4):
        arrive(REST + i)
    for i, t in enumerate(steps):
        for r in (O, M) if t >= LATE else (M,):
            gate_up(REST + i, t, r, r)
    for i in range(2):
        fetch_dn(REST + i + SLOTS, DN - 2 + i)
    combine(1, 1)

    def rows_to_mate(n):
        return remote(stage.at[n], xv.at[pl.ds(R, ROWS), pl.ds(n * W, W)], p_send.at[n], p_recv.at[n], mate)

    def write(n):
        return pltpu.make_async_copy(stage.at[n], y_hbm.at[:, pl.ds(n * W, W)], osem.at[n])

    def each(what, *steps):
        for n in steps:
            what(n)

    def send_rows(n):
        rows_to_mate(n).start()

    def take(n):
        rows_to_mate(n).wait()
        to_peer(0, n).wait_recv()
        to_peer(1, n).wait_recv()

    def total(n):
        for h in range(2):
            r = slice(h * HALF, (h + 1) * HALF)
            mates = xv[R + h * HALF : R + (h + 1) * HALF, n * W : (n + 1) * W].astype(F32)
            y = keep[n % 6, r] + mates + sums(h, n)[...].astype(F32)
            stage[n, r] = y.astype(BF16)

    def write_out(n):
        write(n).start()

    def mates_rows(n):
        for w in range(2):
            term = dot(hid[M:R, :], ring[(LAST + n) % SLOTS, w])
            stage[n, :, w * T : (w + 1) * T] = term.astype(BF16)

    def own_rows(n):
        for w in range(2):
            keep[n % 6, :, w * T : (w + 1) * T] = dot(hid[O:M, :], ring[(LAST + n) % SLOTS, w])

    def arrived(n):
        arrive(LAST + n)

    each(arrived, 0, 1, 2, 3)
    send_sums(1, 1)
    each(mates_rows, 0, 1, 2, 3)
    each(own_rows, 0, 1, 2, 3)

    each(send_rows, 0, 1, 2, 3)
    each(arrived, 4, 5)
    each(mates_rows, 4, 5)
    each(own_rows, 4, 5)

    each(send_rows, 4, 5)
    each(take, 0, 1, 2, 3)
    each(arrived, 6, 7)
    each(total, 0, 1, 2, 3)
    each(mates_rows, 6, 7)

    each(send_rows, 6, 7)
    each(write_out, 0, 1, 2, 3)
    each(take, 4, 5)
    each(total, 4, 5)
    each(own_rows, 6, 7)

    each(write_out, 4, 5)
    each(take, 6, 7)
    each(total, 6, 7)
    each(write_out, 6, 7)

    for h in range(2):
        for n in range(DN):
            to_peer(h, n).wait_send()
    for n in range(DN):
        write(n).wait()


def move(y_ref, out_ref, buf, into, out):
    parts = range(4)
    rows = ROWS // len(parts)

    def load(i):
        return pltpu.make_async_copy(y_ref.at[pl.ds(i * rows, rows)], buf.at[i], into.at[i])

    def store(i):
        return pltpu.make_async_copy(buf.at[i], out_ref.at[pl.ds(i * rows, rows)], out.at[i])

    for i in parts:
        load(i).start()
    for i in parts:
        load(i).wait()
        store(i).start()
    for i in parts:
        store(i).wait()


def solution(mesh):
    def step(x, w_gate, w_up, w_down):
        dma = pltpu.SemaphoreType.DMA
        hbm = pl.BlockSpec(memory_space=pltpu.HBM)
        y = pl.pallas_call(
            kernel,
            out_shape=jax.ShapeDtypeStruct((ROWS, D), BF16),
            in_specs=[pl.BlockSpec(memory_space=pltpu.HBM)] * 4,
            out_specs=pl.BlockSpec(memory_space=pltpu.HBM),
            scratch_shapes=[
                pltpu.VMEM((4 * ROWS, D), BF16),
                pltpu.VMEM((3 * ROWS, D), BF16),
                pltpu.VMEM((SLOTS, 2, D, T), BF16),
                pltpu.VMEM((6, ROWS, W), F32),
                pltpu.VMEM((DN, ROWS, W), BF16),
                pltpu.VMEM((DN, HALF, W), BF16),
                pltpu.VMEM((DN, HALF, W), BF16),
                dma((SLOTS, 2)),
                dma,
                dma((DN,)),
                dma((5,)),
                dma((5,)),
                dma((2 * DN,)),
                dma((2 * DN,)),
                dma((2 * DN,)),
                dma((2 * DN,)),
                dma((DN,)),
                dma((DN,)),
                pltpu.SemaphoreType.REGULAR((2,)),
            ],
            compiler_params=pltpu.CompilerParams(
                collective_id=0, has_side_effects=True, vmem_limit_bytes=67043328
            ),
            name="mlp",
        )(x, w_gate, w_up, w_down)
        return pl.pallas_call(
            move,
            out_shape=jax.ShapeDtypeStruct((ROWS, D), BF16),
            in_specs=[hbm],
            out_specs=hbm,
            scratch_shapes=[pltpu.VMEM((4, ROWS // 4, D), BF16), dma((4,)), dma((4,))],
            name="move",
        )(y)

    return jax.shard_map(
        step,
        mesh=mesh,
        in_specs=(P(("dp", "tp"), None), P(None, "tp"), P(None, "tp"), P("tp", None)),
        out_specs=P(("dp", "tp"), None),
        check_vma=False,
    )
```

```python
import jax
import jax.numpy as jnp
from jax import lax
from jax.experimental import pallas as pl
from jax.experimental.pallas import tpu as pltpu
from jax.sharding import PartitionSpec as P

MESH = pl.DeviceIdType.MESH
BF16, F32 = jnp.bfloat16, jnp.float32
D = 4096
ROWS = 256
HALF = ROWS // 2
T = 256
W = 2 * T
GU, DN = D // T, D // W
SLOTS = 10
LEFT = 2
LATE = GU - 2
PASS = GU + DN
REST = LATE + 2 * PASS
LAST = REST + GU - LATE + LEFT
O, M, R = 0, ROWS, 2 * ROWS


def dot(a, b):
    return jnp.dot(a, b, preferred_element_type=F32)


def kernel(
    x_hbm, wg_hbm, wu_hbm, wd_hbm, stage,
    xv, hid, ring, keep, drecv, yrecv,
    wsem, xsem, ag_send, ag_recv, d_send, d_recv, i_send, i_recv, p_send, p_recv, free,
):
    dp, tp = lax.axis_index("dp"), lax.axis_index("tp")
    chip, core = tp // 2, tp % 2
    mate = (dp, chip * 2 + 1 - core)
    peer = (dp, (1 - chip) * 2 + core)

    def remote(src, dst, send, recv, to):
        return pltpu.make_async_remote_copy(
            src_ref=src, dst_ref=dst, send_sem=send, recv_sem=recv, device_id=to, device_id_type=MESH
        )

    def tile(ref, t, slot, which):
        return pltpu.make_async_copy(
            ref.at[:, pl.ds(pl.multiple_of(t * T, T), T)], ring.at[slot, which], wsem.at[slot, which]
        )

    def fetch_gu(q, t):
        slot = lax.rem(q, SLOTS)
        tile(wg_hbm, t, slot, 0).start()
        tile(wu_hbm, t, slot, 1).start()

    def fetch_dn(q, n):
        slot = lax.rem(q, SLOTS)
        tile(wd_hbm, 2 * n, slot, 0).start()
        tile(wd_hbm, 2 * n + 1, slot, 1).start()

    def arrive(q):
        slot = lax.rem(q, SLOTS)
        tile(wg_hbm, 0, slot, 0).wait()
        tile(wg_hbm, 0, slot, 1).wait()

    def gate_up(q, t, row, out):
        slot = lax.rem(q, SLOTS)
        x = xv[pl.ds(row, ROWS), :]
        gate = dot(x, ring[slot, 0])
        up = dot(x, ring[slot, 1])
        hid[pl.ds(out, ROWS), pl.ds(pl.multiple_of(t * T, T), T)] = (jax.nn.silu(gate) * up).astype(BF16)

    own = pltpu.make_async_copy(x_hbm, xv.at[pl.ds(O, ROWS)], xsem)
    own.start()
    for q in range(3):
        fetch_gu(q, q)
    barrier = pltpu.get_barrier_semaphore()
    for to in (mate, peer):
        pl.semaphore_signal(barrier, inc=1, device_id=to, device_id_type=MESH)
    pl.semaphore_wait(barrier, 2)
    near = remote(x_hbm, xv.at[pl.ds(M, ROWS)], ag_send.at[0], ag_recv.at[0], mate)
    near.start()

    def far(h):
        return remote(
            x_hbm.at[pl.ds(h * HALF, HALF)], xv.at[pl.ds(R + h * ROWS, HALF)], ag_send.at[1 + h], ag_recv.at[1 + h], peer
        )

    def forward(h):
        return remote(
            xv.at[pl.ds(R + h * ROWS, HALF)],
            xv.at[pl.ds(R + h * ROWS + HALF, HALF)],
            ag_send.at[3 + h], ag_recv.at[3 + h], mate,
        )

    far(0).start()
    far(1).start()
    own.wait()

    def pass_own(q, _):
        arrive(q)
        gate_up(q, q, O, O)
        for i in range(2):
            fetch_gu(2 * q + 3 + i, 2 * q + 3 + i)
        return 0

    lax.fori_loop(0, LEFT, pass_own, 0)
    near.wait()

    def pass_near(q, u):
        for i in range(u):
            arrive(q + i)
        for i in range(u):
            gate_up(q + i, q + i, O, O)
            gate_up(q + i, q + i, M, M)

    def pass_single(q, _):
        pass_near(q, 1)
        for i in range(3):
            fetch_gu(3 * q + 1 + i, 3 * q + 1 + i)
        pl.when(q == LEFT + 1)(lambda: fetch_gu(LATE - 1, LATE - 1))
        return 0

    lax.fori_loop(LEFT, LEFT + 2, pass_single, 0)

    def pass_double(j, _):
        @pl.when(j == LATE // 2 - 1)
        def _():
            far(0).wait_recv()
            forward(0).start()

        q = 2 * j
        pass_near(q, 2)
        for i in range(2):
            fetch_gu(q + i + SLOTS, lax.rem(q + i + SLOTS, LATE))
        return 0

    lax.fori_loop(LEFT // 2 + 1, LATE // 2, pass_double, 0)
    forward(0).wait()

    def place(n, part):
        return pl.ds(R + ROWS + part * HALF, HALF), pl.ds(n * W, W)

    def terms(h, n):
        return xv.at[place(n, 0)] if h else drecv.at[n]

    def sums(h, n):
        return xv.at[place(n, 1)] if h else yrecv.at[n]

    def to_mate(h, d, i):
        n = 4 * d + i
        k = h * DN + n
        src = stage.at[pl.ds(i % 2 * HALF, HALF), pl.ds((2 * d + i // 2) * W, W)]
        return remote(src, terms(h, n), d_send.at[k], d_recv.at[k], mate)

    def to_peer(h, n):
        k = h * DN + n
        return remote(terms(h, n), sums(h, n), i_send.at[k], i_recv.at[k], peer)

    def send_terms(h, d):
        for i in range(4):
            to_mate(h, d, i).start()

    def combine(h, d):
        for i in range(4):
            to_mate(h, d, i).wait()
        for i in range(4):
            at = terms(h, 4 * d + i)
            mine = keep[2 * d + i // 2, i % 2 * HALF : (i % 2 + 1) * HALF]
            at[...] = (mine + at[...].astype(F32)).astype(BF16)

    def send_sums(h, d):
        for i in range(4):
            to_peer(h, 4 * d + i).start()

    def half(h, _):
        base = LATE + PASS * h
        row = pl.multiple_of(R + h * ROWS, ROWS)

        def gate_up_far(j, _):
            q = base + 4 * j

            @pl.when(jnp.logical_and(h == 1, j == 0))
            def _():
                combine(0, 0)
                send_terms(0, 1)
                send_sums(0, 0)

            @pl.when(jnp.logical_and(h == 1, j == 1))
            def _():
                combine(0, 1)

            for i in range(4):
                arrive(q + i)

            @pl.when(jnp.logical_and(h == 1, j == 1))
            def _():
                send_sums(0, 1)

            for i in range(4):
                gate_up(q + i, 4 * j + i, row, R)

            @pl.when(j < 2)
            def _():
                for i in range(2):
                    fetch_gu(q + i + SLOTS, 4 * j + i + SLOTS)

            @pl.when(j >= 2)
            def _():
                for i in range(2):
                    fetch_dn(q + i + SLOTS, 4 * j + i + SLOTS - GU)

            @pl.when(j < 1)
            def _():
                for i in range(2, 4):
                    fetch_gu(q + i + SLOTS, 4 * j + i + SLOTS)

            @pl.when(jnp.logical_and(j >= 1, j < 3))
            def _():
                for i in range(2, 4):
                    fetch_dn(q + i + SLOTS, 4 * j + i + SLOTS - GU)

            @pl.when(j == 3)
            def _():
                for i in range(2):
                    fetch_gu(q + i + 2 + SLOTS, LATE * h + i)

            return 0

        lax.fori_loop(0, GU // 4, gate_up_far, 0)

        @pl.when(h == 0)
        def _():
            far(1).wait_recv()
            forward(1).start()

        @pl.when(h == 1)
        def _():
            for i, to in enumerate((mate, peer)):
                pl.semaphore_signal(free.at[i], inc=1, device_id=to, device_id_type=MESH)

        def down_far(d, _):
            q = base + GU + 4 * d

            @pl.when(jnp.logical_and(d == 1, h == 0))
            def _():
                send_terms(0, 0)

            @pl.when(jnp.logical_and(d == 1, h == 1))
            def _():
                pl.semaphore_wait(free.at[0], 1)
                send_terms(1, 0)

            for i in range(4):
                arrive(q + i)
            for i in range(4):
                slot = lax.rem(q + i, SLOTS)
                r = slice(i % 2 * HALF, (i % 2 + 1) * HALF)
                for w in range(2):
                    c = slice(w * T, (w + 1) * T)
                    term = dot(hid[R:, :], ring[slot, w])
                    keep[2 * d + i // 2, r, c] = term[:HALF]
                    at = pl.multiple_of((2 * d + i // 2) * W + w * T, T)
                    stage[r, pl.ds(at, T)] = term[HALF:].astype(BF16)

            @pl.when(h == 0)
            def _():
                for i in range(4):
                    fetch_gu(q + i + SLOTS, 4 * d + i + 2)

            @pl.when(jnp.logical_and(h == 1, d == 0))
            def _():
                for i in range(2):
                    fetch_gu(q + i + SLOTS, i)
                for i in range(2):
                    fetch_dn(q + i + 2 + SLOTS, i)

            @pl.when(jnp.logical_and(h == 1, d == 1))
            def _():
                for i in range(4):
                    fetch_dn(q + i + SLOTS, i + 2)

            return 0

        lax.fori_loop(0, DN // 4, down_far, 0)

        @pl.when(h == 0)
        def _():
            forward(1).wait()

        return 0

    lax.fori_loop(0, 2, half, 0)
    far(0).wait_send()
    far(1).wait_send()

    combine(1, 0)
    send_terms(1, 1)
    pl.semaphore_wait(free.at[1], 1)
    send_sums(1, 0)
    steps = (*range(LATE, GU), *range(LEFT))
    for i in range(4):
        arrive(REST + i)
    for i, t in enumerate(steps):
        for r in (O, M) if t >= LATE else (M,):
            gate_up(REST + i, t, r, r)
    for i in range(2):
        fetch_dn(REST + i + SLOTS, DN - 2 + i)
    combine(1, 1)

    def rows_to_mate(n):
        c = pl.ds(n * W, W)
        return remote(stage.at[:, c], xv.at[pl.ds(R, ROWS), c], p_send.at[n], p_recv.at[n], mate)

    def each(what, *steps):
        for n in steps:
            what(n)

    def send_rows(n):
        rows_to_mate(n).start()

    def take(n):
        rows_to_mate(n).wait()
        to_peer(0, n).wait_recv()
        to_peer(1, n).wait_recv()

    def total(n):
        for h in range(2):
            r = slice(h * HALF, (h + 1) * HALF)
            mates = xv[R + h * HALF : R + (h + 1) * HALF, n * W : (n + 1) * W].astype(F32)
            y = keep[n % 6, r] + mates + sums(h, n)[...].astype(F32)
            stage[r, n * W : (n + 1) * W] = y.astype(BF16)

    def mates_rows(n):
        for w in range(2):
            term = dot(hid[M:R, :], ring[(LAST + n) % SLOTS, w])
            stage[:, n * W + w * T : n * W + (w + 1) * T] = term.astype(BF16)

    def own_rows(n):
        for w in range(2):
            keep[n % 6, :, w * T : (w + 1) * T] = dot(hid[O:M, :], ring[(LAST + n) % SLOTS, w])

    def arrived(n):
        arrive(LAST + n)

    each(arrived, 0, 1, 2, 3)
    send_sums(1, 1)
    each(mates_rows, 0, 1, 2, 3)
    each(own_rows, 0, 1, 2, 3)

    each(send_rows, 0, 1, 2, 3)
    each(arrived, 4, 5)
    each(mates_rows, 4, 5)
    each(own_rows, 4, 5)

    each(send_rows, 4, 5)
    each(take, 0, 1, 2, 3)
    each(arrived, 6, 7)
    each(total, 0, 1, 2, 3)
    each(mates_rows, 6, 7)

    each(send_rows, 6, 7)
    each(take, 4, 5)
    each(total, 4, 5)
    each(own_rows, 6, 7)

    each(take, 6, 7)
    each(total, 6, 7)

    for h in range(2):
        for n in range(DN):
            to_peer(h, n).wait_send()


def solution(mesh):
    def step(x, w_gate, w_up, w_down):
        dma = pltpu.SemaphoreType.DMA
        hbm = pl.BlockSpec(memory_space=pltpu.HBM)
        return pl.pallas_call(
            kernel,
            out_shape=pltpu.VMEM((ROWS, D), BF16),
            in_specs=[hbm] * 4,
            out_specs=pl.BlockSpec(memory_space=pltpu.VMEM),
            scratch_shapes=[
                pltpu.VMEM((4 * ROWS, D), BF16),
                pltpu.VMEM((3 * ROWS, D), BF16),
                pltpu.VMEM((SLOTS, 2, D, T), BF16),
                pltpu.VMEM((6, ROWS, W), F32),
                pltpu.VMEM((DN, HALF, W), BF16),
                pltpu.VMEM((DN, HALF, W), BF16),
                dma((SLOTS, 2)),
                dma,
                dma((5,)),
                dma((5,)),
                dma((2 * DN,)),
                dma((2 * DN,)),
                dma((2 * DN,)),
                dma((2 * DN,)),
                dma((DN,)),
                dma((DN,)),
                pltpu.SemaphoreType.REGULAR((2,)),
            ],
            compiler_params=pltpu.CompilerParams(
                collective_id=0, has_side_effects=True, vmem_limit_bytes=123 * 2**19
            ),
            name="mlp",
        )(x, w_gate, w_up, w_down)

    return jax.shard_map(
        step,
        mesh=mesh,
        in_specs=(P(("dp", "tp"), None), P(None, "tp"), P(None, "tp"), P("tp", None)),
        out_specs=P(("dp", "tp"), None),
        check_vma=False,
    )
```

```python
import jax
import jax.numpy as jnp
from jax import lax
from jax.experimental import pallas as pl
from jax.experimental.pallas import tpu as pltpu
from jax.sharding import PartitionSpec as P

MESH = pl.DeviceIdType.MESH
BF16, F32 = jnp.bfloat16, jnp.float32
D = 4096
ROWS = 256
HALF = ROWS // 2
T = 256
W = 2 * T
GU, DN = D // T, D // W
SLOTS = 10
LEFT = 2
LATE = GU - 2
PASS = GU + DN
REST = LATE + 2 * PASS
LAST = REST + GU - LATE + LEFT
O, M, R = 0, ROWS, 2 * ROWS


def dot(a, b):
    return jnp.dot(a, b, preferred_element_type=F32)


def kernel(
    x_hbm, wg_hbm, wu_hbm, wd_hbm, stage,
    xv, hid, ring, keep, drecv, yrecv,
    wsem, xsem, ag_send, ag_recv, d_send, d_recv, i_send, i_recv, p_send, p_recv, free,
):
    dp, tp = lax.axis_index("dp"), lax.axis_index("tp")
    chip, core = tp // 2, tp % 2
    mate = (dp, chip * 2 + 1 - core)
    peer = (dp, (1 - chip) * 2 + core)

    def remote(src, dst, send, recv, to):
        return pltpu.make_async_remote_copy(
            src_ref=src, dst_ref=dst, send_sem=send, recv_sem=recv, device_id=to, device_id_type=MESH
        )

    def tile(ref, t, slot, which):
        return pltpu.make_async_copy(
            ref.at[:, pl.ds(pl.multiple_of(t * T, T), T)], ring.at[slot, which], wsem.at[slot, which]
        )

    def fetch_gu(q, t):
        slot = lax.rem(q, SLOTS)
        tile(wg_hbm, t, slot, 0).start()
        tile(wu_hbm, t, slot, 1).start()

    def fetch_dn(q, n):
        slot = lax.rem(q, SLOTS)
        tile(wd_hbm, 2 * n, slot, 0).start()
        tile(wd_hbm, 2 * n + 1, slot, 1).start()

    def arrive(q):
        slot = lax.rem(q, SLOTS)
        tile(wg_hbm, 0, slot, 0).wait()
        tile(wg_hbm, 0, slot, 1).wait()

    def gate_up(q, t, row, out):
        slot = lax.rem(q, SLOTS)
        x = xv[pl.ds(row, ROWS), :]
        gate = dot(x, ring[slot, 0])
        up = dot(x, ring[slot, 1])
        hid[pl.ds(out, ROWS), pl.ds(pl.multiple_of(t * T, T), T)] = (jax.nn.silu(gate) * up).astype(BF16)

    own = pltpu.make_async_copy(x_hbm, xv.at[pl.ds(O, ROWS)], xsem)
    own.start()
    for q in range(2):
        fetch_gu(q, q)
    barrier = pltpu.get_barrier_semaphore()
    for to in (mate, peer):
        pl.semaphore_signal(barrier, inc=1, device_id=to, device_id_type=MESH)
    pl.semaphore_wait(barrier, 2)
    near = remote(x_hbm, xv.at[pl.ds(M, ROWS)], ag_send.at[0], ag_recv.at[0], mate)
    near.start()

    def far(h):
        return remote(
            x_hbm.at[pl.ds(h * HALF, HALF)], xv.at[pl.ds(R + h * ROWS, HALF)], ag_send.at[1 + h], ag_recv.at[1 + h], peer
        )

    def forward(h):
        return remote(
            xv.at[pl.ds(R + h * ROWS, HALF)],
            xv.at[pl.ds(R + h * ROWS + HALF, HALF)],
            ag_send.at[3 + h], ag_recv.at[3 + h], mate,
        )

    far(0).start()
    far(1).start()
    for q in range(2, SLOTS):
        fetch_gu(q, q)
    own.wait()

    def pass_own(q, _):
        arrive(q)
        gate_up(q, q, O, O)
        fetch_gu(q + SLOTS, q + SLOTS)
        return 0

    lax.fori_loop(0, LEFT, pass_own, 0)
    near.wait()

    def pass_near(q, u):
        for i in range(u):
            arrive(q + i)
        for i in range(u):
            gate_up(q + i, q + i, O, O)
            gate_up(q + i, q + i, M, M)

    def pass_single(q, _):
        pass_near(q, 1)
        fetch_gu(q + SLOTS, q + SLOTS)
        return 0

    lax.fori_loop(LEFT, LEFT + 2, pass_single, 0)

    def pass_double(j, _):
        @pl.when(j == LATE // 2 - 1)
        def _():
            far(0).wait_recv()
            forward(0).start()

        q = 2 * j
        pass_near(q, 2)
        for i in range(2):
            fetch_gu(q + i + SLOTS, lax.rem(q + i + SLOTS, LATE))
        return 0

    lax.fori_loop(LEFT // 2 + 1, LATE // 2, pass_double, 0)
    forward(0).wait()

    def place(n, part):
        return pl.ds(R + ROWS + part * HALF, HALF), pl.ds(n * W, W)

    def terms(h, n):
        return xv.at[place(n, 0)] if h else drecv.at[n]

    def sums(h, n):
        return xv.at[place(n, 1)] if h else yrecv.at[n]

    def to_mate(h, d, i):
        n = 4 * d + i
        k = h * DN + n
        src = stage.at[pl.ds(i % 2 * HALF, HALF), pl.ds((2 * d + i // 2) * W, W)]
        return remote(src, terms(h, n), d_send.at[k], d_recv.at[k], mate)

    def to_peer(h, n):
        k = h * DN + n
        return remote(terms(h, n), sums(h, n), i_send.at[k], i_recv.at[k], peer)

    def send_terms(h, d):
        for i in range(4):
            to_mate(h, d, i).start()

    def combine(h, d):
        for i in range(4):
            to_mate(h, d, i).wait()
        for i in range(4):
            at = terms(h, 4 * d + i)
            mine = keep[2 * d + i // 2, i % 2 * HALF : (i % 2 + 1) * HALF]
            at[...] = (mine + at[...].astype(F32)).astype(BF16)

    def send_sums(h, d):
        for i in range(4):
            to_peer(h, 4 * d + i).start()

    def half(h, _):
        base = LATE + PASS * h
        row = pl.multiple_of(R + h * ROWS, ROWS)

        def gate_up_far(j, _):
            q = base + 4 * j

            @pl.when(jnp.logical_and(h == 1, j == 0))
            def _():
                combine(0, 0)
                send_terms(0, 1)
                send_sums(0, 0)

            @pl.when(jnp.logical_and(h == 1, j == 1))
            def _():
                combine(0, 1)

            for i in range(4):
                arrive(q + i)

            @pl.when(jnp.logical_and(h == 1, j == 1))
            def _():
                send_sums(0, 1)

            for i in range(4):
                gate_up(q + i, 4 * j + i, row, R)

            @pl.when(j < 2)
            def _():
                for i in range(2):
                    fetch_gu(q + i + SLOTS, 4 * j + i + SLOTS)

            @pl.when(j >= 2)
            def _():
                for i in range(2):
                    fetch_dn(q + i + SLOTS, 4 * j + i + SLOTS - GU)

            @pl.when(j < 1)
            def _():
                for i in range(2, 4):
                    fetch_gu(q + i + SLOTS, 4 * j + i + SLOTS)

            @pl.when(jnp.logical_and(j >= 1, j < 3))
            def _():
                for i in range(2, 4):
                    fetch_dn(q + i + SLOTS, 4 * j + i + SLOTS - GU)

            @pl.when(j == 3)
            def _():
                for i in range(2):
                    fetch_gu(q + i + 2 + SLOTS, LATE * h + i)

            return 0

        lax.fori_loop(0, GU // 4, gate_up_far, 0)

        @pl.when(h == 0)
        def _():
            far(1).wait_recv()
            forward(1).start()

        @pl.when(h == 1)
        def _():
            for i, to in enumerate((mate, peer)):
                pl.semaphore_signal(free.at[i], inc=1, device_id=to, device_id_type=MESH)

        def down_far(d, _):
            q = base + GU + 4 * d

            @pl.when(jnp.logical_and(d == 1, h == 0))
            def _():
                send_terms(0, 0)

            @pl.when(jnp.logical_and(d == 1, h == 1))
            def _():
                pl.semaphore_wait(free.at[0], 1)
                send_terms(1, 0)

            for i in range(4):
                arrive(q + i)
            for i in range(4):
                slot = lax.rem(q + i, SLOTS)
                r = slice(i % 2 * HALF, (i % 2 + 1) * HALF)
                for w in range(2):
                    c = slice(w * T, (w + 1) * T)
                    term = dot(hid[R:, :], ring[slot, w])
                    keep[2 * d + i // 2, r, c] = term[:HALF]
                    at = pl.multiple_of((2 * d + i // 2) * W + w * T, T)
                    stage[r, pl.ds(at, T)] = term[HALF:].astype(BF16)

            @pl.when(h == 0)
            def _():
                for i in range(4):
                    fetch_gu(q + i + SLOTS, 4 * d + i + 2)

            @pl.when(jnp.logical_and(h == 1, d == 0))
            def _():
                for i in range(2):
                    fetch_gu(q + i + SLOTS, i)
                for i in range(2):
                    fetch_dn(q + i + 2 + SLOTS, i)

            @pl.when(jnp.logical_and(h == 1, d == 1))
            def _():
                for i in range(4):
                    fetch_dn(q + i + SLOTS, i + 2)

            return 0

        lax.fori_loop(0, DN // 4, down_far, 0)

        @pl.when(h == 0)
        def _():
            forward(1).wait()

        return 0

    lax.fori_loop(0, 2, half, 0)
    far(0).wait_send()
    far(1).wait_send()

    combine(1, 0)
    send_terms(1, 1)
    pl.semaphore_wait(free.at[1], 1)
    send_sums(1, 0)
    steps = (*range(LATE, GU), *range(LEFT))
    for i in range(4):
        arrive(REST + i)
    for i, t in enumerate(steps):
        for r in (O, M) if t >= LATE else (M,):
            gate_up(REST + i, t, r, r)
    for i in range(2):
        fetch_dn(REST + i + SLOTS, DN - 2 + i)
    combine(1, 1)

    def rows_to_mate(n):
        c = pl.ds(n * W, W)
        return remote(stage.at[:, c], xv.at[pl.ds(R, ROWS), c], p_send.at[n], p_recv.at[n], mate)

    def each(what, *steps):
        for n in steps:
            what(n)

    def send_rows(n):
        rows_to_mate(n).start()

    def take(n):
        rows_to_mate(n).wait()
        to_peer(0, n).wait_recv()
        to_peer(1, n).wait_recv()

    def total(n):
        for h in range(2):
            r = slice(h * HALF, (h + 1) * HALF)
            mates = xv[R + h * HALF : R + (h + 1) * HALF, n * W : (n + 1) * W].astype(F32)
            y = keep[n % 6, r] + mates + sums(h, n)[...].astype(F32)
            stage[r, n * W : (n + 1) * W] = y.astype(BF16)

    def mates_rows(n):
        for w in range(2):
            term = dot(hid[M:R, :], ring[(LAST + n) % SLOTS, w])
            stage[:, n * W + w * T : n * W + (w + 1) * T] = term.astype(BF16)

    def own_rows(n):
        for w in range(2):
            keep[n % 6, :, w * T : (w + 1) * T] = dot(hid[O:M, :], ring[(LAST + n) % SLOTS, w])

    def arrived(n):
        arrive(LAST + n)

    each(arrived, 0, 1, 2, 3)
    send_sums(1, 1)
    each(mates_rows, 0, 1, 2, 3)
    each(own_rows, 0, 1, 2, 3)

    each(send_rows, 0, 1, 2, 3)
    each(arrived, 4, 5)
    each(mates_rows, 4, 5)
    each(own_rows, 4, 5)

    each(send_rows, 4, 5)
    each(take, 0, 1, 2, 3)
    each(arrived, 6, 7)
    each(total, 0, 1, 2, 3)
    each(mates_rows, 6, 7)

    each(send_rows, 6, 7)
    each(take, 4, 5)
    each(total, 4, 5)
    each(own_rows, 6, 7)

    each(take, 6, 7)
    each(total, 6, 7)

    for h in range(2):
        for n in range(DN):
            to_peer(h, n).wait_send()


def solution(mesh):
    def step(x, w_gate, w_up, w_down):
        dma = pltpu.SemaphoreType.DMA
        hbm = pl.BlockSpec(memory_space=pltpu.HBM)
        return pl.pallas_call(
            kernel,
            out_shape=pltpu.VMEM((ROWS, D), BF16),
            in_specs=[hbm] * 4,
            out_specs=pl.BlockSpec(memory_space=pltpu.VMEM),
            scratch_shapes=[
                pltpu.VMEM((4 * ROWS, D), BF16),
                pltpu.VMEM((3 * ROWS, D), BF16),
                pltpu.VMEM((SLOTS, 2, D, T), BF16),
                pltpu.VMEM((6, ROWS, W), F32),
                pltpu.VMEM((DN, HALF, W), BF16),
                pltpu.VMEM((DN, HALF, W), BF16),
                dma((SLOTS, 2)),
                dma,
                dma((5,)),
                dma((5,)),
                dma((2 * DN,)),
                dma((2 * DN,)),
                dma((2 * DN,)),
                dma((2 * DN,)),
                dma((DN,)),
                dma((DN,)),
                pltpu.SemaphoreType.REGULAR((2,)),
            ],
            compiler_params=pltpu.CompilerParams(
                collective_id=0, has_side_effects=True, vmem_limit_bytes=123 * 2**19
            ),
            name="mlp",
        )(x, w_gate, w_up, w_down)

    return jax.shard_map(
        step,
        mesh=mesh,
        in_specs=(P(("dp", "tp"), None), P(None, "tp"), P(None, "tp"), P("tp", None)),
        out_specs=P(("dp", "tp"), None),
        check_vma=False,
    )
```
